256 devices in a mesh: rows: 16 (over y, x_lo, core), cols: 4 (over z_1, x_hi), slabs: 2 (over z_0), trial: 2 (over z_2).
Axes of the slice: x: 4 (x_hi: 2, x_lo: 2; x = x_hi * 2 + x_lo), y: 4, z: 8 (z_0: 2, z_1: 2, z_2: 2; z = z_0 * 4 + z_1 * 2 + z_2), core: 2. Of those that a mesh axis runs over, the one named last changes fastest.
Arguments:
- field_values: float32 [256, 64, 128, 128], P(('trial', 'rows'), 'cols', 'slabs'), parts along dimension 0, may hold values from 0.2 to 1.8
- crowding: float32 [256, 64, 128, 128], P(('trial', 'rows'), 'cols', 'slabs'), parts along dimension 0, may hold values from 0.5 to 2
Outputs:
- potential: float32 [256, 64, 128, 128], P(('trial', 'rows'), 'cols', 'slabs'), parts along dimension 0
- field_values_end: float32 [256, 64, 128, 128], P(('trial', 'rows'), 'cols', 'slabs'), parts along dimension 0
The draws below stay inside these ranges and needn't reach their ends.
There are 2 independent parts, one for each index of `trial`. The reference program is written for one: setup_inputs(seed, part) draws one part's arguments, and reference() takes and returns one part's arrays. A program takes and returns all parts, laid end to end along the dimension named above; each array names one. Nothing has to cross between parts.
All inputs are finite; a program needn't handle non-finite values.
Results may differ from the reference program's by a relative error of at most 0.00002.
Values sent between devices are 32-bit elements; how exact they have to be, the bound alone decides.
No kernel may reach another device: no remote copies, remote signals or barrier semaphores. Data moves between devices by JAX's collectives and lax.ppermute only.
A program may use at most 64 MiB of HBM per device.

```python
import jax
import jax.numpy as jnp
from jax import lax

GRID_J = 128
GRID_I = 64
GRID_K = 128
LEVELS = 128
STEPS = 3


def block_levels(rng, shape, pieces, least, top_value):
    factor_of = 1.0
    for axis_at, parts in pieces:
        steps = jax.random.uniform(jax.random.fold_in(jax.random.fold_in(rng, 6), axis_at), (parts,), jnp.float32, least / len(pieces), top_value / len(pieces))
        factor_of = factor_of * jnp.repeat(jnp.exp(steps), shape[axis_at] // parts).reshape((-1,) + (1,) * (len(shape) - 1 - axis_at))
    return factor_of


def setup_inputs(seed: int = 0, part: int = 0) -> dict:
    keys = jax.random.split(jax.random.key(seed), 3)
    part_splits = jax.random.split(jax.random.fold_in(keys[2], part), 3)
    return {
        "field_values": jnp.clip(0.2 + 1.5999999 * jax.random.uniform(part_splits[0], (GRID_J, GRID_I, GRID_K, LEVELS), jnp.float32) ** block_levels(part_splits[0], (GRID_J, GRID_I, GRID_K, LEVELS), ((0, 16), (1, 4), (2, 2)), -0.2, 0.2), 0.2, 1.8),
        "crowding": jnp.clip(0.5 + 1.5 * jax.random.uniform(part_splits[1], (GRID_J, GRID_I, GRID_K, LEVELS), jnp.float32) ** block_levels(part_splits[1], (GRID_J, GRID_I, GRID_K, LEVELS), ((0, 16), (1, 4), (2, 2)), -0.2, 0.2), 0.5, 2.0),
    }


def without_rim(values, dims):
    for dim in dims:
        values = lax.slice_in_dim(values, 1, values.shape[dim] - 1, axis=dim)
    return values


def shifted_cells(values, dim, start, dims):
    others = [other for other in dims if other != dim]
    values = without_rim(values, others)
    return lax.slice_in_dim(values, start, start + values.shape[dim] - 2, axis=dim)


def march_step(padded, crowding):
    middle = without_rim(padded, (0, 1, 2))
    lower = [shifted_cells(padded, dim, 0, (0, 1, 2)) for dim in (0, 1, 2)]
    upper = [shifted_cells(padded, dim, 2, (0, 1, 2)) for dim in (0, 1, 2)]
    spread = lower[0] + upper[0] + lower[1] + upper[1] + lower[2] + upper[2] - 6.0 * middle
    return middle + 0.1 * spread + 0.2 * middle * (1.0 - middle * crowding)


def reference(field_values, crowding):
    for step in range(STEPS):
        field_values = march_step(jnp.pad(field_values, ((1, 1), (1, 1), (1, 1), (0, 0)), mode="constant"), crowding)
    potential = jnp.cumsum(field_values, axis=0) / GRID_J
    return potential, field_values
```

```python
import functools

import jax
import jax.numpy as jnp
from jax import lax
from jax.experimental import pallas as pl
from jax.experimental.pallas import tpu as pltpu
from jax.sharding import PartitionSpec as P


STEPS = 3
HALF = 64
TILE = 8
VMEM = pl.BlockSpec(memory_space=pltpu.MemorySpace.VMEM)
SMEM = pl.BlockSpec(memory_space=pltpu.MemorySpace.SMEM)


def call(body, outs, args, scratch=(), limit=16, **more):
    return pl.pallas_call(
        body,
        out_shape=[jax.ShapeDtypeStruct(s, jnp.float32) for s in outs],
        scratch_shapes=[pltpu.VMEM(s, jnp.float32) for s in scratch],
        compiler_params=pltpu.CompilerParams(vmem_limit_bytes=limit * 1024 * 1024),
        **more,
    )(*args)


def left(shape=(TILE, 128)):
    return lax.broadcasted_iota(jnp.int32, shape, len(shape) - 1) < HALF


def swap(v):
    return pltpu.roll(v, HALF, v.ndim - 1)


def pack_tiles(ref, j, i, t, nk):
    a = ref[j, i, pl.ds(t * TILE, TILE), :]
    b = ref[j, i, pl.ds(nk // 2 + t * TILE, TILE), :]
    m = left()
    return jnp.where(m, a, swap(b)), jnp.where(m, swap(a), b)


def write_faces(place, out, s_c0, s_c1, s_k):
    nj, ni, nk = out.shape[:3]
    for j in range(nj):
        first, last = out[j, 0], out[j, ni - 1]
        s_c0[j] = jnp.where(place[1] == 0, last, first)
        s_c1[j] = jnp.where(place[1] == 0, first, last)
        s_k[j] = jnp.where(place[2] == 0, out[j, :, nk - 1, :], out[j, :, 0, :])


def pack_field(place, f, fa, fb, *faces):
    nj, ni, nk = f.shape[:3]
    sa, sb = faces[:5], faces[5:]

    def at(i, _):
        for t in range(nk // 2 // TILE):
            ends = {}
            for j in range(nj):
                a, b = pack_tiles(f, j, i, t, nk)
                fa[j, i, pl.ds(t * TILE, TILE), :] = a
                fb[j, i, pl.ds(t * TILE, TILE), :] = b
                if j in (0, nj - 1):
                    ends[j] = (a, b)
            for n, s in ((0, sa), (1, sb)):
                first, last = ends[0][n], ends[nj - 1][n]
                s[0][i, pl.ds(t * TILE, TILE), :] = jnp.where(place[0] == 0, last, first)
                s[1][i, pl.ds(t * TILE, TILE), :] = jnp.where(place[0] == 0, first, last)
        return 0

    lax.fori_loop(0, ni, at, 0)
    write_faces(place, fa, *sa[2:])
    write_faces(place, fb, *sb[2:])


def pack_crowding(c, ca, cb):
    nj, ni, nk = c.shape[:3]

    def at(i, _):
        for j in range(nj):
            for t in range(nk // 2 // TILE):
                a, b = pack_tiles(c, j, i, t, nk)
                ca[j, i, pl.ds(t * TILE, TILE), :] = 0.2 * a
                cb[j, i, pl.ds(t * TILE, TILE), :] = 0.2 * b
        return 0

    lax.fori_loop(0, ni, at, 0)


def step_body(last, with_total, place, f, c, r0, r1, c0, c1, ks, *rest):
    rest = list(rest)
    earlier = rest.pop(0) if with_total else None
    out = rest.pop(0)
    if last:
        total = rest.pop(0)
    else:
        s_r0, s_r1, s_c0, s_c1, s_k = rest[:5]
        rest = rest[5:]
    kl, kh = rest
    nj, ni, nk = f.shape[:3]
    tiles = nk // TILE
    wide = left((ni, 128))
    for j in range(nj):
        x = swap(ks[j])
        low_side = jnp.where(place[2] == 1, x, 0.0)
        high_side = jnp.where(place[2] == 0, x, 0.0)
        kl[j] = jnp.where(wide, low_side, swap(f[j, :, nk - 1, :]))
        kh[j] = jnp.where(wide, swap(f[j, :, 0, :]), high_side)
    row = lax.broadcasted_iota(jnp.int32, (TILE, 128), 0)
    top, bottom = row == 0, row == TILE - 1
    even_r, even_c = place[0] == 0, place[1] == 0

    def ds(t):
        return pl.ds(t * TILE, TILE)

    def at(i, below, above):
        down = [jnp.where(even_r, r1[i, ds(t), :], r0[i, ds(t), :]) for t in range(tiles)]
        mid = [f[0, i, ds(t), :] for t in range(tiles)]
        sums, first = [None] * tiles, [None] * tiles
        for j in range(nj):
            if j + 1 < nj:
                up = [f[j + 1, i, ds(t), :] for t in range(tiles)]
            else:
                up = [jnp.where(even_r, r0[i, ds(t), :], r1[i, ds(t), :]) for t in range(tiles)]
            fwd = [pltpu.roll(v, 1, 0) for v in mid]
            bwd = [pltpu.roll(v, TILE - 1, 0) for v in mid]
            low = jnp.broadcast_to(kl[j, pl.ds(i, 1), :], (TILE, 128))
            high = jnp.broadcast_to(kh[j, pl.ds(i, 1), :], (TILE, 128))
            for t in range(tiles):
                before = jnp.where(top, fwd[t - 1] if t else low, fwd[t])
                after = jnp.where(bottom, bwd[t + 1] if t + 1 < tiles else high, bwd[t])
                around = (down[t] + up[t]) + (below(j, t) + above(j, t)) + (before + after)
                v = mid[t] * (0.6 - c[j, i, ds(t), :] * mid[t]) + 0.1 * around
                out[j, i, ds(t), :] = v
                if last:
                    sums[t] = v if j == 0 else sums[t] + v
                elif j == 0:
                    first[t] = v
                elif j == nj - 1:
                    s_r0[i, ds(t), :] = jnp.where(even_r, v, first[t])
                    s_r1[i, ds(t), :] = jnp.where(even_r, first[t], v)
            down, mid = mid, up
        if last:
            base = nk if with_total else 0
            for t in range(tiles):
                total[i, pl.ds(base + t * TILE, TILE), :] = sums[t]
                if with_total:
                    total[i, ds(t), :] = earlier[i, ds(t), :]

    def inner(i, _):
        at(i, lambda j, t: f[j, i - 1, ds(t), :], lambda j, t: f[j, i + 1, ds(t), :])
        return 0

    at(0, lambda j, t: jnp.where(even_c, c1[j, ds(t), :], c0[j, ds(t), :]), lambda j, t: f[j, 1, ds(t), :])
    lax.fori_loop(1, ni - 1, inner, 0)
    at(ni - 1, lambda j, t: f[j, ni - 2, ds(t), :], lambda j, t: jnp.where(even_c, c0[j, ds(t), :], c1[j, ds(t), :]))
    if not last:
        write_faces(place, out, s_c0, s_c1, s_k)


def prefix_body(g, out):
    n = g.shape[0]
    state = jnp.zeros(g.shape[1:], jnp.float32)
    for d in range(n):
        out[d] = state
        if d + 1 < n:
            state = state + g[d]


def finish_body(scale, fa, fb, base, potential, field):
    nj, _, nk = fa.shape[:3]
    m = left()
    for t in range(nk // TILE):
        lo, hi = pl.ds(t * TILE, TILE), pl.ds(nk + t * TILE, TILE)

        def both(a, b):
            return jnp.where(m, a, swap(b)), jnp.where(m, swap(a), b)

        acc0, acc1 = both(base[0, lo, :], base[0, hi, :])
        for j in range(nj):
            v0, v1 = both(fa[j, 0, lo, :], fb[j, 0, lo, :])
            field[j, 0, lo, :] = v0
            field[j, 0, hi, :] = v1
            acc0, acc1 = acc0 + v0, acc1 + v1
            potential[j, 0, lo, :] = acc0 * scale
            potential[j, 0, hi, :] = acc1 * scale


def pairs(size, start):
    out = []
    for i in range(start, size - 1, 2):
        out += [(i, i + 1), (i + 1, i)]
    return out


KINDS = ("k", "c1", "c0", "r0", "r1")


def exchange(faces):
    r0, r1, c0, c1, k = faces
    rows, cols, slabs = lax.axis_size("rows"), lax.axis_size("cols"), lax.axis_size("slabs")
    sends = {
        "k": (k, "slabs", pairs(slabs, 0)),
        "c0": (c0, "cols", pairs(cols, 0)),
        "c1": (c1, "cols", pairs(cols, 1)),
        "r0": (r0, "rows", pairs(rows, 0)),
        "r1": (r1, "rows", pairs(rows, 1)),
    }
    got = {}
    for kind in KINDS:
        got[kind] = lax.ppermute(*sends[kind])
    return [got[kind] for kind in ("r0", "r1", "c0", "c1", "k")]


def on_device(field_values, crowding):
    nj, ni, nk, nl = field_values.shape
    half = (nj, ni, nk // 2, nl)
    faces = [(ni, nk // 2, nl)] * 2 + [(nj, nk // 2, nl)] * 2 + [(nj, ni, nl)]
    place = jnp.stack([lax.axis_index("rows") % 2, lax.axis_index("cols") % 2, lax.axis_index("slabs")])
    place = place.astype(jnp.int32)
    out = call(
        pack_field, [half, half] + faces + faces, (place, field_values), in_specs=[SMEM, VMEM]
    )
    f, sent = [out[0], out[1]], [out[2:7], out[7:12]]
    halos = [exchange(sent[0]), exchange(sent[1])]
    c = call(pack_crowding, [half, half], (crowding,))
    scratch = [(nj, ni, nl)] * 2
    total = None
    for step in range(STEPS):
        last = step == STEPS - 1
        for h in range(2):
            with_total = last and h == 1
            args = (place, f[h], c[h], *halos[h]) + ((total,) if with_total else ())
            if last:
                outs = [half, (ni, nk if with_total else nk // 2, nl)]
            else:
                outs = [half] + faces
            res = call(
                functools.partial(step_body, last, with_total),
                outs,
                args,
                scratch,
                in_specs=[SMEM] + [VMEM] * (len(args) - 1),
            )
            f[h] = res[0]
            if last:
                total = res[1]
            else:
                halos[h] = exchange(res[1:])
    rows = lax.axis_size("rows")
    gathered = lax.all_to_all(total.reshape(rows, ni * nk // rows, nl), "rows", 0, 0, tiled=True)
    before = call(prefix_body, [gathered.shape], (gathered,))[0]
    base = lax.all_to_all(before, "rows", 0, 0, tiled=True).reshape(ni, nk, nl)
    full = pl.BlockSpec((nj, 1, nk, nl), lambda i: (0, i, 0, 0))
    part = pl.BlockSpec((nj, 1, nk // 2, nl), lambda i: (0, i, 0, 0))
    potential, field = call(
        functools.partial(finish_body, 1.0 / (nj * rows)),
        [field_values.shape] * 2,
        (f[0], f[1], base),
        grid=(ni,),
        in_specs=[part, part, pl.BlockSpec((1, nk, nl), lambda i: (i, 0, 0))],
        out_specs=[full, full],
    )
    return potential, field


def solution(mesh):
    spec = P(("trial", "rows"), "cols", "slabs", None)
    return jax.shard_map(
        on_device, mesh=mesh, in_specs=(spec, spec), out_specs=(spec, spec), check_vma=False
    )
```

```python
import functools

import jax
import jax.numpy as jnp
from jax import lax
from jax.experimental import pallas as pl
from jax.experimental.pallas import tpu as pltpu
from jax.sharding import PartitionSpec as P


STEPS = 3
HALF = 64
TILE = 8
VMEM = pl.BlockSpec(memory_space=pltpu.MemorySpace.VMEM)
SMEM = pl.BlockSpec(memory_space=pltpu.MemorySpace.SMEM)


def call(body, outs, args, scratch=(), limit=16, **more):
    return pl.pallas_call(
        body,
        out_shape=[jax.ShapeDtypeStruct(s, jnp.float32) for s in outs],
        scratch_shapes=[pltpu.VMEM(s, jnp.float32) for s in scratch],
        compiler_params=pltpu.CompilerParams(vmem_limit_bytes=limit * 1024 * 1024),
        **more,
    )(*args)


def left(shape=(TILE, 128)):
    return lax.broadcasted_iota(jnp.int32, shape, len(shape) - 1) < HALF


def swap(v):
    return pltpu.roll(v, HALF, v.ndim - 1)


def pack_tiles(ref, j, i, t, nk):
    a = ref[j, i, pl.ds(t * TILE, TILE), :]
    b = ref[j, i, pl.ds(nk // 2 + t * TILE, TILE), :]
    m = left()
    return jnp.where(m, a, swap(b)), jnp.where(m, swap(a), b)


def write_faces(place, out, s_c0, s_c1, s_k):
    nj, ni, nk = out.shape[:3]
    for j in range(nj):
        first, last = out[j, 0], out[j, ni - 1]
        s_c0[j] = jnp.where(place[1] == 0, last, first)
        s_c1[j] = jnp.where(place[1] == 0, first, last)
        s_k[j] = jnp.where(place[2] == 0, out[j, :, nk - 1, :], out[j, :, 0, :])


def pack_field(place, f, fa, fb, *faces):
    nj, ni, nk = f.shape[:3]
    sa, sb = faces[:5], faces[5:]

    def at(i, _):
        for t in range(nk // 2 // TILE):
            ends = {}
            for j in range(nj):
                a, b = pack_tiles(f, j, i, t, nk)
                fa[j, i, pl.ds(t * TILE, TILE), :] = a
                fb[j, i, pl.ds(t * TILE, TILE), :] = b
                if j in (0, nj - 1):
                    ends[j] = (a, b)
            for n, s in ((0, sa), (1, sb)):
                first, last = ends[0][n], ends[nj - 1][n]
                s[0][i, pl.ds(t * TILE, TILE), :] = jnp.where(place[0] == 0, last, first)
                s[1][i, pl.ds(t * TILE, TILE), :] = jnp.where(place[0] == 0, first, last)
        return 0

    lax.fori_loop(0, ni, at, 0)
    write_faces(place, fa, *sa[2:])
    write_faces(place, fb, *sb[2:])


def pack_crowding(c, ca, cb):
    nj, ni, nk = c.shape[:3]

    def at(i, _):
        for j in range(nj):
            for t in range(nk // 2 // TILE):
                a, b = pack_tiles(c, j, i, t, nk)
                ca[j, i, pl.ds(t * TILE, TILE), :] = 0.2 * a
                cb[j, i, pl.ds(t * TILE, TILE), :] = 0.2 * b
        return 0

    lax.fori_loop(0, ni, at, 0)


def step_body(last, with_total, place, f, c, r0, r1, c0, c1, ks, *rest):
    rest = list(rest)
    earlier = rest.pop(0) if with_total else None
    out = rest.pop(0)
    if last:
        total = rest.pop(0)
    else:
        s_r0, s_r1, s_c0, s_c1, s_k = rest[:5]
        rest = rest[5:]
    kl, kh = rest
    nj, ni, nk = f.shape[:3]
    tiles = nk // TILE
    wide = left((ni, 128))
    for j in range(nj):
        x = swap(ks[j])
        low_side = jnp.where(place[2] == 1, x, 0.0)
        high_side = jnp.where(place[2] == 0, x, 0.0)
        kl[j] = jnp.where(wide, low_side, swap(f[j, :, nk - 1, :]))
        kh[j] = jnp.where(wide, swap(f[j, :, 0, :]), high_side)
    row = lax.broadcasted_iota(jnp.int32, (TILE, 128), 0)
    top, bottom = row == 0, row == TILE - 1
    even_r, even_c = place[0] == 0, place[1] == 0

    def ds(t):
        return pl.ds(t * TILE, TILE)

    def at(i, below, above):
        down = [jnp.where(even_r, r1[i, ds(t), :], r0[i, ds(t), :]) for t in range(tiles)]
        mid = [f[0, i, ds(t), :] for t in range(tiles)]
        sums, first = [None] * tiles, [None] * tiles
        for j in range(nj):
            if j + 1 < nj:
                up = [f[j + 1, i, ds(t), :] for t in range(tiles)]
            else:
                up = [jnp.where(even_r, r0[i, ds(t), :], r1[i, ds(t), :]) for t in range(tiles)]
            fwd = [pltpu.roll(v, 1, 0) for v in mid]
            bwd = [pltpu.roll(v, TILE - 1, 0) for v in mid]
            low = jnp.broadcast_to(kl[j, pl.ds(i, 1), :], (TILE, 128))
            high = jnp.broadcast_to(kh[j, pl.ds(i, 1), :], (TILE, 128))
            for t in range(tiles):
                before = jnp.where(top, fwd[t - 1] if t else low, fwd[t])
                after = jnp.where(bottom, bwd[t + 1] if t + 1 < tiles else high, bwd[t])
                around = (down[t] + up[t]) + (below(j, t) + above(j, t)) + (before + after)
                v = mid[t] * (0.6 - c[j, i, ds(t), :] * mid[t]) + 0.1 * around
                out[j, i, ds(t), :] = v
                if last:
                    sums[t] = v if j == 0 else sums[t] + v
                elif j == 0:
                    first[t] = v
                elif j == nj - 1:
                    s_r0[i, ds(t), :] = jnp.where(even_r, v, first[t])
                    s_r1[i, ds(t), :] = jnp.where(even_r, first[t], v)
            down, mid = mid, up
        if last:
            base = nk if with_total else 0
            for t in range(tiles):
                total[i, pl.ds(base + t * TILE, TILE), :] = sums[t]
                if with_total:
                    total[i, ds(t), :] = earlier[i, ds(t), :]

    def inner(i, _):
        at(i, lambda j, t: f[j, i - 1, ds(t), :], lambda j, t: f[j, i + 1, ds(t), :])
        return 0

    at(0, lambda j, t: jnp.where(even_c, c1[j, ds(t), :], c0[j, ds(t), :]), lambda j, t: f[j, 1, ds(t), :])
    lax.fori_loop(1, ni - 1, inner, 0)
    at(ni - 1, lambda j, t: f[j, ni - 2, ds(t), :], lambda j, t: jnp.where(even_c, c0[j, ds(t), :], c1[j, ds(t), :]))
    if not last:
        write_faces(place, out, s_c0, s_c1, s_k)


def prefix_body(g, out):
    n = g.shape[0]
    state = jnp.zeros(g.shape[1:], jnp.float32)
    for d in range(n):
        out[d] = state
        if d + 1 < n:
            state = state + g[d]


GROUP = 2


def finish_body(scale, fa, fb, base, potential, field, pot, end, sems):
    nj, ni, nk = fa.shape[:3]
    m = left()

    def both(a, b):
        return jnp.where(m, a, swap(b)), jnp.where(m, swap(a), b)

    def copies(g):
        part = pl.ds(g * GROUP, GROUP)
        return (
            pltpu.make_async_copy(pot.at[:, part], potential.at[:, part], sems.at[g, 0]),
            pltpu.make_async_copy(end.at[:, part], field.at[:, part], sems.at[g, 1]),
        )

    def at(g, _):
        for n in range(GROUP):
            i = g * GROUP + n
            for t in range(nk // TILE):
                lo, hi = pl.ds(t * TILE, TILE), pl.ds(nk + t * TILE, TILE)
                acc0, acc1 = both(base[i, lo, :], base[i, hi, :])
                for j in range(nj):
                    v0, v1 = both(fa[j, i, lo, :], fb[j, i, lo, :])
                    end[j, i, lo, :] = v0
                    end[j, i, hi, :] = v1
                    acc0, acc1 = acc0 + v0, acc1 + v1
                    pot[j, i, lo, :] = acc0 * scale
                    pot[j, i, hi, :] = acc1 * scale
        for copy in copies(g):
            copy.start()
        return 0

    def finished(g, _):
        for copy in copies(g):
            copy.wait()
        return 0

    lax.fori_loop(0, ni // GROUP, at, 0)
    lax.fori_loop(0, ni // GROUP, finished, 0)


def pairs(size, start):
    out = []
    for i in range(start, size - 1, 2):
        out += [(i, i + 1), (i + 1, i)]
    return out


KINDS = ("r1", "c1", "k", "c0", "r0")


def exchange(faces):
    r0, r1, c0, c1, k = faces
    rows, cols, slabs = lax.axis_size("rows"), lax.axis_size("cols"), lax.axis_size("slabs")
    sends = {
        "k": (k, "slabs", pairs(slabs, 0)),
        "c0": (c0, "cols", pairs(cols, 0)),
        "c1": (c1, "cols", pairs(cols, 1)),
        "r0": (r0, "rows", pairs(rows, 0)),
        "r1": (r1, "rows", pairs(rows, 1)),
    }
    got = {}
    for kind in KINDS:
        got[kind] = lax.ppermute(*sends[kind])
    return [got[kind] for kind in ("r0", "r1", "c0", "c1", "k")]


def on_device(field_values, crowding):
    nj, ni, nk, nl = field_values.shape
    half = (nj, ni, nk // 2, nl)
    faces = [(ni, nk // 2, nl)] * 2 + [(nj, nk // 2, nl)] * 2 + [(nj, ni, nl)]
    place = jnp.stack([lax.axis_index("rows") % 2, lax.axis_index("cols") % 2, lax.axis_index("slabs")])
    place = place.astype(jnp.int32)
    out = call(
        pack_field, [half, half] + faces + faces, (place, field_values), in_specs=[SMEM, VMEM]
    )
    f, sent = [out[0], out[1]], [out[2:7], out[7:12]]
    halos = [exchange(sent[0]), exchange(sent[1])]
    c = call(pack_crowding, [half, half], (crowding,))
    scratch = [(nj, ni, nl)] * 2
    total = None
    for step in range(STEPS):
        last = step == STEPS - 1
        for h in range(2):
            with_total = last and h == 1
            args = (place, f[h], c[h], *halos[h]) + ((total,) if with_total else ())
            if last:
                outs = [half, (ni, nk if with_total else nk // 2, nl)]
            else:
                outs = [half] + faces
            res = call(
                functools.partial(step_body, last, with_total),
                outs,
                args,
                scratch,
                in_specs=[SMEM] + [VMEM] * (len(args) - 1),
            )
            f[h] = res[0]
            if last:
                total = res[1]
            else:
                halos[h] = exchange(res[1:])
    rows = lax.axis_size("rows")
    gathered = lax.all_to_all(total.reshape(rows, ni * nk // rows, nl), "rows", 0, 0, tiled=True)
    before = call(prefix_body, [gathered.shape], (gathered,))[0]
    base = lax.all_to_all(before, "rows", 0, 0, tiled=True).reshape(ni, nk, nl)
    potential, field = pl.pallas_call(
        functools.partial(finish_body, 1.0 / (nj * rows)),
        out_shape=[jax.ShapeDtypeStruct(field_values.shape, jnp.float32)] * 2,
        in_specs=[VMEM] * 3,
        out_specs=[pl.BlockSpec(memory_space=pltpu.MemorySpace.HBM)] * 2,
        scratch_shapes=[pltpu.VMEM(field_values.shape, jnp.float32)] * 2
        + [pltpu.SemaphoreType.DMA((ni // GROUP, 2))],
        compiler_params=pltpu.CompilerParams(vmem_limit_bytes=16 * 1024 * 1024),
    )(f[0], f[1], base)
    return potential, field


def solution(mesh):
    spec = P(("trial", "rows"), "cols", "slabs", None)
    return jax.shard_map(
        on_device, mesh=mesh, in_specs=(spec, spec), out_specs=(spec, spec), check_vma=False
    )
```

```python
import functools

import jax
import jax.numpy as jnp
from jax import lax
from jax.experimental import pallas as pl
from jax.experimental.pallas import tpu as pltpu
from jax.sharding import PartitionSpec as P


STEPS = 3
HALF = 64
TILE = 8
VMEM = pl.BlockSpec(memory_space=pltpu.MemorySpace.VMEM)
SMEM = pl.BlockSpec(memory_space=pltpu.MemorySpace.SMEM)


def call(body, outs, args, scratch=(), limit=16, **more):
    return pl.pallas_call(
        body,
        out_shape=[jax.ShapeDtypeStruct(s, jnp.float32) for s in outs],
        scratch_shapes=[pltpu.VMEM(s, jnp.float32) for s in scratch],
        compiler_params=pltpu.CompilerParams(vmem_limit_bytes=limit * 1024 * 1024),
        **more,
    )(*args)


def left(shape=(TILE, 128)):
    return lax.broadcasted_iota(jnp.int32, shape, len(shape) - 1) < HALF


def swap(v):
    return pltpu.roll(v, HALF, v.ndim - 1)


def pack_tiles(ref, j, i, t, nk):
    a = ref[j, i, pl.ds(t * TILE, TILE), :]
    b = ref[j, i, pl.ds(nk // 2 + t * TILE, TILE), :]
    m = left()
    return jnp.where(m, a, swap(b)), jnp.where(m, swap(a), b)


def edge_rows(place, block, j):
    nk = block.shape[2]
    return jnp.where(place[2] == 0, block[j, :, nk - 1, :], block[j, :, 0, :])


def write_faces(place, out, s_c0, s_c1, s_k, other):
    nj, ni = out.shape[:2]
    wide = left((ni, 128))
    for j in range(nj):
        first, last = out[j, 0], out[j, ni - 1]
        s_c0[j] = jnp.where(place[1] == 0, last, first)
        s_c1[j] = jnp.where(place[1] == 0, first, last)
        rows = edge_rows(place, out, j)
        if other is not None:
            mine = swap(rows)
            rows = jnp.where(place[2] == 0, jnp.where(wide, mine, other[j]), jnp.where(wide, other[j], mine))
        s_k[j] = rows


def pack_field(place, f, fa, fb, *faces):
    nj, ni, nk = f.shape[:3]
    sa, sb = faces[:5], faces[5:]

    def at(i, _):
        for t in range(nk // 2 // TILE):
            ends = {}
            for j in range(nj):
                a, b = pack_tiles(f, j, i, t, nk)
                fa[j, i, pl.ds(t * TILE, TILE), :] = a
                fb[j, i, pl.ds(t * TILE, TILE), :] = b
                if j in (0, nj - 1):
                    ends[j] = (a, b)
            for n, s in ((0, sa), (1, sb)):
                first, last = ends[0][n], ends[nj - 1][n]
                s[0][i, pl.ds(t * TILE, TILE), :] = jnp.where(place[0] == 0, last, first)
                s[1][i, pl.ds(t * TILE, TILE), :] = jnp.where(place[0] == 0, first, last)
        return 0

    lax.fori_loop(0, ni, at, 0)
    write_faces(place, fa, *sa[2:], None)
    write_faces(place, fb, *sb[2:], sa[4])


def pack_crowding(c, ca, cb):
    nj, ni, nk = c.shape[:3]

    def at(i, _):
        for j in range(nj):
            for t in range(nk // 2 // TILE):
                a, b = pack_tiles(c, j, i, t, nk)
                ca[j, i, pl.ds(t * TILE, TILE), :] = 0.2 * a
                cb[j, i, pl.ds(t * TILE, TILE), :] = 0.2 * b
        return 0

    lax.fori_loop(0, ni, at, 0)


def step_body(last, h, place, f, c, r0, r1, c0, c1, ks, *rest):
    rest = list(rest)
    earlier = rest.pop(0) if h else None
    with_total = last and h == 1
    out = rest.pop(0)
    if last:
        total = rest.pop(0)
    else:
        s_r0, s_r1, s_c0, s_c1, s_k = rest[:5]
        rest = rest[5:]
    kl, kh = rest
    nj, ni, nk = f.shape[:3]
    tiles = nk // TILE
    wide = left((ni, 128))
    for j in range(nj):
        x = ks[j] if h else swap(ks[j])
        low_side = jnp.where(place[2] == 1, x, 0.0)
        high_side = jnp.where(place[2] == 0, x, 0.0)
        kl[j] = jnp.where(wide, low_side, swap(f[j, :, nk - 1, :]))
        kh[j] = jnp.where(wide, swap(f[j, :, 0, :]), high_side)
    row = lax.broadcasted_iota(jnp.int32, (TILE, 128), 0)
    top, bottom = row == 0, row == TILE - 1
    even_r, even_c = place[0] == 0, place[1] == 0

    def ds(t):
        return pl.ds(t * TILE, TILE)

    def at(i, below, above):
        down = [jnp.where(even_r, r1[i, ds(t), :], r0[i, ds(t), :]) for t in range(tiles)]
        mid = [f[0, i, ds(t), :] for t in range(tiles)]
        sums, first = [None] * tiles, [None] * tiles
        for j in range(nj):
            if j + 1 < nj:
                up = [f[j + 1, i, ds(t), :] for t in range(tiles)]
            else:
                up = [jnp.where(even_r, r0[i, ds(t), :], r1[i, ds(t), :]) for t in range(tiles)]
            fwd = [pltpu.roll(v, 1, 0) for v in mid]
            bwd = [pltpu.roll(v, TILE - 1, 0) for v in mid]
            low = jnp.broadcast_to(kl[j, pl.ds(i, 1), :], (TILE, 128))
            high = jnp.broadcast_to(kh[j, pl.ds(i, 1), :], (TILE, 128))
            for t in range(tiles):
                before = jnp.where(top, fwd[t - 1] if t else low, fwd[t])
                after = jnp.where(bottom, bwd[t + 1] if t + 1 < tiles else high, bwd[t])
                around = (down[t] + up[t]) + (below(j, t) + above(j, t)) + (before + after)
                v = mid[t] * (0.6 - c[j, i, ds(t), :] * mid[t]) + 0.1 * around
                out[j, i, ds(t), :] = v
                if last:
                    sums[t] = v if j == 0 else sums[t] + v
                elif j == 0:
                    first[t] = v
                elif j == nj - 1:
                    s_r0[i, ds(t), :] = jnp.where(even_r, v, first[t])
                    s_r1[i, ds(t), :] = jnp.where(even_r, first[t], v)
            down, mid = mid, up
        if last:
            base = nk if with_total else 0
            for t in range(tiles):
                total[i, pl.ds(base + t * TILE, TILE), :] = sums[t]
                if with_total:
                    total[i, ds(t), :] = earlier[i, ds(t), :]

    def inner(i, _):
        at(i, lambda j, t: f[j, i - 1, ds(t), :], lambda j, t: f[j, i + 1, ds(t), :])
        return 0

    at(0, lambda j, t: jnp.where(even_c, c1[j, ds(t), :], c0[j, ds(t), :]), lambda j, t: f[j, 1, ds(t), :])
    lax.fori_loop(1, ni - 1, inner, 0)
    at(ni - 1, lambda j, t: f[j, ni - 2, ds(t), :], lambda j, t: jnp.where(even_c, c0[j, ds(t), :], c1[j, ds(t), :]))
    if not last:
        write_faces(place, out, s_c0, s_c1, s_k, earlier)


def prefix_body(g, out):
    n = g.shape[0]
    state = jnp.zeros(g.shape[1:], jnp.float32)
    for d in range(n):
        out[d] = state
        if d + 1 < n:
            state = state + g[d]


GROUP = 2


def finish_body(scale, fa, fb, base, potential, field, pot, end, sems):
    nj, ni, nk = fa.shape[:3]
    m = left()

    def both(a, b):
        return jnp.where(m, a, swap(b)), jnp.where(m, swap(a), b)

    def copies(g):
        part = pl.ds(g * GROUP, GROUP)
        return (
            pltpu.make_async_copy(pot.at[:, part], potential.at[:, part], sems.at[g, 0]),
            pltpu.make_async_copy(end.at[:, part], field.at[:, part], sems.at[g, 1]),
        )

    def at(g, _):
        for n in range(GROUP):
            i = g * GROUP + n
            for t in range(nk // TILE):
                lo, hi = pl.ds(t * TILE, TILE), pl.ds(nk + t * TILE, TILE)
                acc0, acc1 = both(base[i, lo, :], base[i, hi, :])
                for j in range(nj):
                    v0, v1 = both(fa[j, i, lo, :], fb[j, i, lo, :])
                    end[j, i, lo, :] = v0
                    end[j, i, hi, :] = v1
                    acc0, acc1 = acc0 + v0, acc1 + v1
                    pot[j, i, lo, :] = acc0 * scale
                    pot[j, i, hi, :] = acc1 * scale
        for copy in copies(g):
            copy.start()
        return 0

    def finished(g, _):
        for copy in copies(g):
            copy.wait()
        return 0

    lax.fori_loop(0, ni // GROUP, at, 0)
    lax.fori_loop(0, ni // GROUP, finished, 0)


def pairs(size, start):
    out = []
    for i in range(start, size - 1, 2):
        out += [(i, i + 1), (i + 1, i)]
    return out


KINDS = (("r1", "c1", "c0", "r0"), ("k", "r1", "c1", "c0", "r0"))


def exchange(faces, h):
    r0, r1, c0, c1, k = faces
    rows, cols, slabs = lax.axis_size("rows"), lax.axis_size("cols"), lax.axis_size("slabs")
    sends = {
        "k": (k, "slabs", pairs(slabs, 0)),
        "c0": (c0, "cols", pairs(cols, 0)),
        "c1": (c1, "cols", pairs(cols, 1)),
        "r0": (r0, "rows", pairs(rows, 0)),
        "r1": (r1, "rows", pairs(rows, 1)),
    }
    got = {}
    for kind in KINDS[h]:
        got[kind] = lax.ppermute(*sends[kind])
    return [got[kind] for kind in ("r0", "r1", "c0", "c1")], got.get("k")


def on_device(field_values, crowding):
    nj, ni, nk, nl = field_values.shape
    half = (nj, ni, nk // 2, nl)
    faces = [(ni, nk // 2, nl)] * 2 + [(nj, nk // 2, nl)] * 2 + [(nj, ni, nl)]
    place = jnp.stack([lax.axis_index("rows") % 2, lax.axis_index("cols") % 2, lax.axis_index("slabs")])
    place = place.astype(jnp.int32)
    out = call(
        pack_field, [half, half] + faces + faces, (place, field_values), in_specs=[SMEM, VMEM]
    )
    f, sent = [out[0], out[1]], [out[2:7], out[7:12]]
    halos = [None, None]
    for h in range(2):
        halos[h], across = exchange(sent[h], h)
    c = call(pack_crowding, [half, half], (crowding,))
    scratch = [(nj, ni, nl)] * 2
    extra = None
    for step in range(STEPS):
        last = step == STEPS - 1
        for h in range(2):
            args = (place, f[h], c[h], *halos[h], across) + ((extra,) if h else ())
            if last:
                outs = [half, (ni, nk if h else nk // 2, nl)]
            else:
                outs = [half] + faces
            res = call(
                functools.partial(step_body, last, h),
                outs,
                args,
                scratch,
                in_specs=[SMEM] + [VMEM] * (len(args) - 1),
            )
            f[h] = res[0]
            extra = res[-1]
            if not last:
                halos[h], got = exchange(res[1:], h)
        if not last:
            across = got
    rows = lax.axis_size("rows")
    gathered = lax.all_to_all(extra.reshape(rows, ni * nk // rows, nl), "rows", 0, 0, tiled=True)
    before = call(prefix_body, [gathered.shape], (gathered,))[0]
    base = lax.all_to_all(before, "rows", 0, 0, tiled=True).reshape(ni, nk, nl)
    potential, field = pl.pallas_call(
        functools.partial(finish_body, 1.0 / (nj * rows)),
        out_shape=[jax.ShapeDtypeStruct(field_values.shape, jnp.float32)] * 2,
        in_specs=[VMEM] * 3,
        out_specs=[pl.BlockSpec(memory_space=pltpu.MemorySpace.HBM)] * 2,
        scratch_shapes=[pltpu.VMEM(field_values.shape, jnp.float32)] * 2
        + [pltpu.SemaphoreType.DMA((ni // GROUP, 2))],
        compiler_params=pltpu.CompilerParams(vmem_limit_bytes=16 * 1024 * 1024),
    )(f[0], f[1], base)
    return potential, field


def solution(mesh):
    spec = P(("trial", "rows"), "cols", "slabs", None)
    return jax.shard_map(on_device, mesh=mesh, in_specs=(spec, spec), out_specs=(spec, spec), check_vma=False)
```

```python
import functools

import jax
import jax.numpy as jnp
from jax import lax
from jax.experimental import pallas as pl
from jax.experimental.pallas import tpu as pltpu
from jax.sharding import PartitionSpec as P


STEPS = 3
HALF = 64
TILE = 8
VMEM = pl.BlockSpec(memory_space=pltpu.MemorySpace.VMEM)
SMEM = pl.BlockSpec(memory_space=pltpu.MemorySpace.SMEM)


def near(args):
    return [pltpu.with_memory_space_constraint(a, pltpu.MemorySpace.VMEM) if a.size > 8 else a for a in args]


def call(body, outs, args, scratch=(), limit=16, **more):
    args = near(args)
    return pl.pallas_call(
        body,
        out_shape=[jax.ShapeDtypeStruct(s, jnp.float32) for s in outs],
        scratch_shapes=[pltpu.VMEM(s, jnp.float32) for s in scratch],
        compiler_params=pltpu.CompilerParams(vmem_limit_bytes=limit * 1024 * 1024),
        **more,
    )(*args)


def left(shape=(TILE, 128)):
    return lax.broadcasted_iota(jnp.int32, shape, len(shape) - 1) < HALF


def swap(v):
    return pltpu.roll(v, HALF, v.ndim - 1)


def exchange_halves(a, b):
    m = left()
    moved = swap(jnp.where(m, b, a))
    return jnp.where(m, a, moved), jnp.where(m, moved, b)


def pack_tiles(ref, j, i, t, nk):
    a = ref[j, i, pl.ds(t * TILE, TILE), :]
    b = ref[j, i, pl.ds(nk // 2 + t * TILE, TILE), :]
    return exchange_halves(a, b)


def edge_rows(place, block, j):
    nk = block.shape[2]
    return jnp.where(place[2] == 0, block[j, :, nk - 1, :], block[j, :, 0, :])


def write_faces(place, out, s_c0, s_c1, s_k, other):
    nj, ni = out.shape[:2]
    wide = left((ni, 128))
    for j in range(nj):
        first, last = out[j, 0], out[j, ni - 1]
        s_c0[j] = jnp.where(place[1] == 0, last, first)
        s_c1[j] = jnp.where(place[1] == 0, first, last)
        rows = edge_rows(place, out, j)
        if other is not None:
            mine = swap(rows)
            rows = jnp.where(place[2] == 0, jnp.where(wide, mine, other[j]), jnp.where(wide, other[j], mine))
        s_k[j] = rows


def pack_field(place, f, fa, fb, *faces):
    nj, ni, nk = f.shape[:3]
    sa, sb = faces[:5], faces[5:]

    def at(i, _):
        for t in range(nk // 2 // TILE):
            ends = {}
            for j in range(nj):
                a, b = pack_tiles(f, j, i, t, nk)
                fa[j, i, pl.ds(t * TILE, TILE), :] = a
                fb[j, i, pl.ds(t * TILE, TILE), :] = b
                if j in (0, nj - 1):
                    ends[j] = (a, b)
            for n, s in ((0, sa), (1, sb)):
                first, last = ends[0][n], ends[nj - 1][n]
                s[0][i, pl.ds(t * TILE, TILE), :] = jnp.where(place[0] == 0, last, first)
                s[1][i, pl.ds(t * TILE, TILE), :] = jnp.where(place[0] == 0, first, last)
        return 0

    lax.fori_loop(0, ni, at, 0)
    write_faces(place, fa, *sa[2:], None)
    write_faces(place, fb, *sb[2:], sa[4])


def pack_crowding(c, ca, cb):
    nj, ni, nk = c.shape[:3]

    def at(i, _):
        for j in range(nj):
            for t in range(nk // 2 // TILE):
                a, b = pack_tiles(c, j, i, t, nk)
                ca[j, i, pl.ds(t * TILE, TILE), :] = 0.2 * a
                cb[j, i, pl.ds(t * TILE, TILE), :] = 0.2 * b
        return 0

    lax.fori_loop(0, ni, at, 0)


def step_body(kind, h, place, f, c, r0, r1, c0, c1, ks, *rest):
    rest = list(rest)
    last, with_sums = kind == "last", kind == "sums"
    earlier = rest.pop(0) if h and not last else None
    out = rest.pop(0)
    if last:
        fix = rest.pop(0)
    else:
        s_r0, s_r1, s_c0, s_c1, s_k = rest[:5]
        rest = rest[5:]
        if with_sums:
            g_sum, f_sum = rest[:2]
            rest = rest[2:]
    kl, kh = rest
    nj, ni, nk = f.shape[:3]
    tiles = nk // TILE
    wide = left((ni, 128))
    for j in range(nj):
        x = ks[j] if h else swap(ks[j])
        low_side = jnp.where(place[2] == 1, x, 0.0)
        high_side = jnp.where(place[2] == 0, x, 0.0)
        kl[j] = jnp.where(wide, low_side, swap(f[j, :, nk - 1, :]))
        kh[j] = jnp.where(wide, swap(f[j, :, 0, :]), high_side)
    row = lax.broadcasted_iota(jnp.int32, (TILE, 128), 0)
    top, bottom = row == 0, row == TILE - 1
    even_r, even_c = place[0] == 0, place[1] == 0

    def ds(t):
        return pl.ds(t * TILE, TILE)

    def at(i, below, above):
        down = [jnp.where(even_r, r1[i, ds(t), :], r0[i, ds(t), :]) for t in range(tiles)]
        mid = [f[0, i, ds(t), :] for t in range(tiles)]
        first, grown, total = [None] * tiles, [None] * tiles, [None] * tiles
        if last:
            for t in range(tiles):
                fix[i, ds(t), :] = jnp.where(place[3] == 0, 0.1 * (mid[t] - down[t]), 0.0)
        for j in range(nj):
            if j + 1 < nj:
                up = [f[j + 1, i, ds(t), :] for t in range(tiles)]
            else:
                up = [jnp.where(even_r, r0[i, ds(t), :], r1[i, ds(t), :]) for t in range(tiles)]
            low = jnp.broadcast_to(kl[j, pl.ds(i, 1), :], (TILE, 128))
            high = jnp.broadcast_to(kh[j, pl.ds(i, 1), :], (TILE, 128))
            for t in range(tiles):
                if t:
                    before = f[j, i, pl.ds(t * TILE - 1, TILE), :]
                else:
                    before = jnp.where(top, low, pltpu.roll(mid[t], 1, 0))
                if t + 1 < tiles:
                    after = f[j, i, pl.ds(t * TILE + 1, TILE), :]
                else:
                    after = jnp.where(bottom, high, pltpu.roll(mid[t], TILE - 1, 0))
                around = (down[t] + up[t]) + (below(j, t) + above(j, t)) + (before + after)
                v = mid[t] * (0.6 - c[j, i, ds(t), :] * mid[t]) + 0.1 * around
                out[j, i, ds(t), :] = v
                if j == 0:
                    first[t] = v
                elif j == nj - 1 and not last:
                    s_r0[i, ds(t), :] = jnp.where(even_r, v, first[t])
                    s_r1[i, ds(t), :] = jnp.where(even_r, first[t], v)
                if with_sums:
                    own = v * (0.6 - c[j, i, ds(t), :] * v)
                    grown[t] = own if j == 0 else grown[t] + own
                    total[t] = v if j == 0 else total[t] + v
            down, mid = mid, up
        if with_sums:
            for t in range(tiles):
                g_sum[i, ds(t), :] = grown[t] - jnp.where(place[3] == 1, 0.1 * first[t], 0.0)
                f_sum[i, ds(t), :] = total[t]

    def inner(i, _):
        at(i, lambda j, t: f[j, i - 1, ds(t), :], lambda j, t: f[j, i + 1, ds(t), :])
        return 0

    at(0, lambda j, t: jnp.where(even_c, c1[j, ds(t), :], c0[j, ds(t), :]), lambda j, t: f[j, 1, ds(t), :])
    lax.fori_loop(1, ni - 1, inner, 0)
    at(ni - 1, lambda j, t: f[j, ni - 2, ds(t), :], lambda j, t: jnp.where(even_c, c0[j, ds(t), :], c1[j, ds(t), :]))
    if not last:
        write_faces(place, out, s_c0, s_c1, s_k, earlier)


def totals_body(place, g_a, s_a, g_b, s_b, c0_a, c1_a, c0_b, c1_b, ks, out, kl, kh):
    ni, nk = g_a.shape[:2]
    nj = ks.shape[0]
    tiles = nk // TILE
    wide = left((ni, 128))
    row = lax.broadcasted_iota(jnp.int32, (TILE, 128), 0)
    top, bottom = row == 0, row == TILE - 1
    even_c = place[1] == 0
    across = ks[0]
    for j in range(1, nj):
        across = across + ks[j]
    for h, (g, s, c0, c1) in enumerate(((g_a, s_a, c0_a, c1_a), (g_b, s_b, c0_b, c1_b))):
        x = across if h else swap(across)
        kl[h] = jnp.where(wide, jnp.where(place[2] == 1, x, 0.0), swap(s[:, nk - 1, :]))
        kh[h] = jnp.where(wide, swap(s[:, 0, :]), jnp.where(place[2] == 0, x, 0.0))
        ends = []
        for t in range(tiles):
            part = pl.ds(t * TILE, TILE)
            sum0, sum1 = c0[0, part, :], c1[0, part, :]
            for j in range(1, nj):
                sum0, sum1 = sum0 + c0[j, part, :], sum1 + c1[j, part, :]
            ends.append((jnp.where(even_c, sum1, sum0), jnp.where(even_c, sum0, sum1)))
        for i in range(ni):
            low = jnp.broadcast_to(kl[h, pl.ds(i, 1), :], (TILE, 128))
            high = jnp.broadcast_to(kh[h, pl.ds(i, 1), :], (TILE, 128))
            for t in range(tiles):
                part = pl.ds(t * TILE, TILE)
                mid = s[i, part, :]
                below = s[i - 1, part, :] if i else ends[t][0]
                above = s[i + 1, part, :] if i + 1 < ni else ends[t][1]
                if t:
                    before = s[i, pl.ds(t * TILE - 1, TILE), :]
                else:
                    before = jnp.where(top, low, pltpu.roll(mid, 1, 0))
                if t + 1 < tiles:
                    after = s[i, pl.ds(t * TILE + 1, TILE), :]
                else:
                    after = jnp.where(bottom, high, pltpu.roll(mid, TILE - 1, 0))
                around = (mid + mid) + (below + above) + (before + after)
                out[i, pl.ds(h * nk + t * TILE, TILE), :] = g[i, part, :] + 0.1 * around


def prefix_body(g, out):
    n = g.shape[0]
    state = jnp.zeros(g.shape[1:], jnp.float32)
    for d in range(n):
        out[d] = state
        if d + 1 < n:
            state = state + g[d]


GROUP = 2


def finish_body(scale, fa, fb, base, fix_a, fix_b, potential, field, pot, end, sems):
    nj, ni, nk = fa.shape[:3]

    def copies(g):
        part = pl.ds(g * GROUP, GROUP)
        return (
            pltpu.make_async_copy(pot.at[:, part], potential.at[:, part], sems.at[g, 0]),
            pltpu.make_async_copy(end.at[:, part], field.at[:, part], sems.at[g, 1]),
        )

    def at(g, _):
        for n in range(GROUP):
            i = g * GROUP + n
            for t in range(nk // TILE):
                lo, hi = pl.ds(t * TILE, TILE), pl.ds(nk + t * TILE, TILE)
                acc0, acc1 = exchange_halves(base[i, lo, :] + fix_a[i, lo, :], base[i, hi, :] + fix_b[i, lo, :])
                for j in range(nj):
                    v0, v1 = exchange_halves(fa[j, i, lo, :], fb[j, i, lo, :])
                    end[j, i, lo, :] = v0
                    end[j, i, hi, :] = v1
                    acc0, acc1 = acc0 + v0, acc1 + v1
                    pot[j, i, lo, :] = acc0 * scale
                    pot[j, i, hi, :] = acc1 * scale
        for copy in copies(g):
            copy.start()
        return 0

    def finished(g, _):
        for copy in copies(g):
            copy.wait()
        return 0

    lax.fori_loop(0, ni // GROUP, at, 0)
    lax.fori_loop(0, ni // GROUP, finished, 0)


def pairs(size, start):
    out = []
    for i in range(start, size - 1, 2):
        out += [(i, i + 1), (i + 1, i)]
    return out


KINDS = (("r1", "c1", "c0", "r0"), ("k", "r1", "c1", "c0", "r0"))
LAST = (("r1", "c1", "c0", "r0"), ("c1", "c0", "k", "r1", "r0"))


def kinds(step, h):
    return (LAST if step == STEPS - 1 else KINDS)[h]


def exchange(faces, step, h):
    r0, r1, c0, c1, k = faces
    rows, cols, slabs = lax.axis_size("rows"), lax.axis_size("cols"), lax.axis_size("slabs")
    sends = {
        "k": (k, "slabs", pairs(slabs, 0)),
        "c0": (c0, "cols", pairs(cols, 0)),
        "c1": (c1, "cols", pairs(cols, 1)),
        "r0": (r0, "rows", pairs(rows, 0)),
        "r1": (r1, "rows", pairs(rows, 1)),
    }
    got = {}
    for kind in kinds(step, h):
        got[kind] = lax.ppermute(*sends[kind])
    return [got[kind] for kind in ("r0", "r1", "c0", "c1")], got.get("k")


def on_device(field_values, crowding):
    nj, ni, nk, nl = field_values.shape
    half = (nj, ni, nk // 2, nl)
    faces = [(ni, nk // 2, nl)] * 2 + [(nj, nk // 2, nl)] * 2 + [(nj, ni, nl)]
    row = lax.axis_index("rows")
    place = jnp.stack([row % 2, lax.axis_index("cols") % 2, lax.axis_index("slabs"), row == 0])
    place = place.astype(jnp.int32)
    out = call(
        pack_field, [half, half] + faces + faces, (place, field_values), in_specs=[SMEM, VMEM]
    )
    f, sent = [out[0], out[1]], [out[2:7], out[7:12]]
    halos = [None, None]
    for h in range(2):
        halos[h], across = exchange(sent[h], 0, h)
    c = call(pack_crowding, [half, half], (crowding,))
    scratch = [(nj, ni, nl)] * 2
    sums, fix, other = [None, None], [None, None], None
    rows = lax.axis_size("rows")
    for step in range(STEPS):
        kind = {STEPS - 1: "last", STEPS - 2: "sums"}.get(step, "plain")
        last = kind == "last"
        if last:
            total = call(
                totals_body,
                [(ni, nk, nl)],
                (place, *sums[0], *sums[1], *halos[0][2:], *halos[1][2:], across),
                [(2, ni, nl)] * 2,
                in_specs=[SMEM] + [VMEM] * 9,
            )[0]
            total = total.reshape(rows, ni * nk // rows, nl)
            gathered = lax.all_to_all(total, "rows", 0, 0, tiled=True)
            gathered, place = lax.optimization_barrier((gathered, place))
            before = call(prefix_body, [gathered.shape], (gathered,))[0]
        for h in range(2):
            args = (place, f[h], c[h], *halos[h], across) + ((other,) if h and not last else ())
            plane = (ni, nk // 2, nl)
            outs = [half] + {"last": [plane], "sums": faces + [plane] * 2, "plain": faces}[kind]
            res = call(
                functools.partial(step_body, kind, h),
                outs,
                args,
                scratch,
                in_specs=[SMEM] + [VMEM] * (len(args) - 1),
            )
            f[h] = res[0]
            if last:
                fix[h] = res[1]
            else:
                sums[h] = res[6:]
                other = res[5]
                halos[h], got = exchange(res[1:6], step + 1, h)
        if not last:
            across = got
    before, *f = lax.optimization_barrier((before, *f))
    base = lax.all_to_all(before, "rows", 0, 0, tiled=True).reshape(ni, nk, nl)
    potential, field = pl.pallas_call(
        functools.partial(finish_body, 1.0 / (nj * rows)),
        out_shape=[jax.ShapeDtypeStruct(field_values.shape, jnp.float32)] * 2,
        in_specs=[VMEM] * 5,
        out_specs=[pl.BlockSpec(memory_space=pltpu.MemorySpace.HBM)] * 2,
        scratch_shapes=[pltpu.VMEM(field_values.shape, jnp.float32)] * 2
        + [pltpu.SemaphoreType.DMA((ni // GROUP, 2))],
        compiler_params=pltpu.CompilerParams(vmem_limit_bytes=16 * 1024 * 1024),
    )(*near([f[0], f[1], base, *fix]))
    return potential, field


def solution(mesh):
    spec = P(("trial", "rows"), "cols", "slabs", None)
    return jax.shard_map(on_device, mesh=mesh, in_specs=(spec, spec), out_specs=(spec, spec), check_vma=False)
```

```python
import functools

import jax
import jax.numpy as jnp
from jax import lax
from jax.experimental import pallas as pl
from jax.experimental.pallas import tpu as pltpu
from jax.sharding import PartitionSpec as P


STEPS = 3
HALF = 64
TILE = 8
VMEM = pl.BlockSpec(memory_space=pltpu.MemorySpace.VMEM)
SMEM = pl.BlockSpec(memory_space=pltpu.MemorySpace.SMEM)


def near(args):
    return [pltpu.with_memory_space_constraint(a, pltpu.MemorySpace.VMEM) if a.size > 8 else a for a in args]


def call(body, outs, args, scratch=(), limit=16, **more):
    args = near(args)
    return pl.pallas_call(
        body,
        out_shape=[jax.ShapeDtypeStruct(s, jnp.float32) for s in outs],
        scratch_shapes=[pltpu.VMEM(s, jnp.float32) for s in scratch],
        compiler_params=pltpu.CompilerParams(vmem_limit_bytes=limit * 1024 * 1024),
        **more,
    )(*args)


def left(shape=(TILE, 128)):
    return lax.broadcasted_iota(jnp.int32, shape, len(shape) - 1) < HALF


def swap(v):
    return pltpu.roll(v, HALF, v.ndim - 1)


def exchange_halves(a, b):
    m = left()
    moved = swap(jnp.where(m, b, a))
    return jnp.where(m, a, moved), jnp.where(m, moved, b)


def pack_tiles(ref, j, i, t, nk):
    a = ref[j, i, pl.ds(t * TILE, TILE), :]
    b = ref[j, i, pl.ds(nk // 2 + t * TILE, TILE), :]
    return exchange_halves(a, b)


def edge_rows(place, block, j):
    nk = block.shape[2]
    return jnp.where(place[2] == 0, block[j, :, nk - 1, :], block[j, :, 0, :])


def write_faces(place, out, s_c0, s_c1, s_k, other):
    nj, ni = out.shape[:2]
    wide = left((ni, 128))
    for j in range(nj):
        first, last = out[j, 0], out[j, ni - 1]
        s_c0[j] = jnp.where(place[1] == 0, last, first)
        s_c1[j] = jnp.where(place[1] == 0, first, last)
        rows = edge_rows(place, out, j)
        if other is not None:
            mine = swap(rows)
            rows = jnp.where(place[2] == 0, jnp.where(wide, mine, other[j]), jnp.where(wide, other[j], mine))
        s_k[j] = rows


def pack_faces(place, f, *rest):
    sa, sb, s_k = rest[:4], rest[4:8], rest[8]
    rlo, rhi, clo, chi, klo, khi, sems = rest[9:]
    nj, ni, nk = f.shape[:3]
    copies = [
        pltpu.make_async_copy(part, into, sems.at[n])
        for n, (part, into) in enumerate(
            (
                (f.at[0], rlo),
                (f.at[nj - 1], rhi),
                (f.at[:, 0], clo),
                (f.at[:, ni - 1], chi),
                (f.at[:, :, pl.ds(0, TILE)], klo),
                (f.at[:, :, pl.ds(nk - TILE, TILE)], khi),
            )
        )
    ]
    for copy in copies:
        copy.start()

    def face(n, low, high, even, slot):
        for t in range(nk // 2 // TILE):
            lo, hi = pl.ds(t * TILE, TILE), pl.ds(nk // 2 + t * TILE, TILE)
            first = exchange_halves(low[n, lo, :], low[n, hi, :])
            last = exchange_halves(high[n, lo, :], high[n, hi, :])
            for s, v, w in zip((sa, sb), first, last):
                s[slot][n, lo, :] = jnp.where(even, w, v)
                s[slot + 1][n, lo, :] = jnp.where(even, v, w)

    def along(pair, _):
        for n in range(2):
            face(2 * pair + n, rlo, rhi, place[0] == 0, 0)
        return 0

    copies[0].wait()
    copies[1].wait()
    lax.fori_loop(0, ni // 2, along, 0)
    for copy in copies[2:]:
        copy.wait()
    for j in range(nj):
        face(j, clo, chi, place[1] == 0, 2)
        s_k[j] = jnp.where(place[2] == 0, swap(khi[j, :, TILE - 1, :]), klo[j, :, 0, :])


def pack_field(f, fa, fb):
    nj, ni, nk = f.shape[:3]

    def at(i, _):
        for j in range(nj):
            for t in range(nk // 2 // TILE):
                a, b = pack_tiles(f, j, i, t, nk)
                fa[j, i, pl.ds(t * TILE, TILE), :] = a
                fb[j, i, pl.ds(t * TILE, TILE), :] = b
        return 0

    lax.fori_loop(0, ni, at, 0)


def pack_crowding(c, ca, cb):
    nj, ni, nk = c.shape[:3]

    def at(i, _):
        for j in range(nj):
            for t in range(nk // 2 // TILE):
                a, b = pack_tiles(c, j, i, t, nk)
                ca[j, i, pl.ds(t * TILE, TILE), :] = 0.2 * a
                cb[j, i, pl.ds(t * TILE, TILE), :] = 0.2 * b
        return 0

    lax.fori_loop(0, ni, at, 0)


def step_body(kind, h, place, f, c, r0, r1, c0, c1, ks, *rest):
    rest = list(rest)
    last, with_sums = kind == "last", kind == "sums"
    earlier = rest.pop(0) if h and not last else None
    out = rest.pop(0)
    if last:
        fix = rest.pop(0)
    else:
        s_r0, s_r1, s_c0, s_c1, s_k = rest[:5]
        rest = rest[5:]
        if with_sums:
            g_sum, f_sum = rest[:2]
            rest = rest[2:]
    kl, kh = rest
    nj, ni, nk = f.shape[:3]
    tiles = nk // TILE
    wide = left((ni, 128))
    for j in range(nj):
        x = ks[j] if h else swap(ks[j])
        low_side = jnp.where(place[2] == 1, x, 0.0)
        high_side = jnp.where(place[2] == 0, x, 0.0)
        kl[j] = jnp.where(wide, low_side, swap(f[j, :, nk - 1, :]))
        kh[j] = jnp.where(wide, swap(f[j, :, 0, :]), high_side)
    row = lax.broadcasted_iota(jnp.int32, (TILE, 128), 0)
    top, bottom = row == 0, row == TILE - 1
    even_r, even_c = place[0] == 0, place[1] == 0

    def ds(t):
        return pl.ds(t * TILE, TILE)

    def at(i, below, above):
        down = [jnp.where(even_r, r1[i, ds(t), :], r0[i, ds(t), :]) for t in range(tiles)]
        mid = [f[0, i, ds(t), :] for t in range(tiles)]
        first, grown, total = [None] * tiles, [None] * tiles, [None] * tiles
        if last:
            for t in range(tiles):
                fix[i, ds(t), :] = jnp.where(place[3] == 0, 0.1 * (mid[t] - down[t]), 0.0)
        for j in range(nj):
            if j + 1 < nj:
                up = [f[j + 1, i, ds(t), :] for t in range(tiles)]
            else:
                up = [jnp.where(even_r, r0[i, ds(t), :], r1[i, ds(t), :]) for t in range(tiles)]
            low = jnp.broadcast_to(kl[j, pl.ds(i, 1), :], (TILE, 128))
            high = jnp.broadcast_to(kh[j, pl.ds(i, 1), :], (TILE, 128))
            for t in range(tiles):
                if t:
                    before = f[j, i, pl.ds(t * TILE - 1, TILE), :]
                else:
                    before = jnp.where(top, low, pltpu.roll(mid[t], 1, 0))
                if t + 1 < tiles:
                    after = f[j, i, pl.ds(t * TILE + 1, TILE), :]
                else:
                    after = jnp.where(bottom, high, pltpu.roll(mid[t], TILE - 1, 0))
                around = (down[t] + up[t]) + (below(j, t) + above(j, t)) + (before + after)
                v = mid[t] * (0.6 - c[j, i, ds(t), :] * mid[t]) + 0.1 * around
                out[j, i, ds(t), :] = v
                if j == 0:
                    first[t] = v
                elif j == nj - 1 and not last:
                    s_r0[i, ds(t), :] = jnp.where(even_r, v, first[t])
                    s_r1[i, ds(t), :] = jnp.where(even_r, first[t], v)
                if with_sums:
                    own = v * (0.6 - c[j, i, ds(t), :] * v)
                    grown[t] = own if j == 0 else grown[t] + own
                    total[t] = v if j == 0 else total[t] + v
            down, mid = mid, up
        if with_sums:
            for t in range(tiles):
                g_sum[i, ds(t), :] = grown[t] - jnp.where(place[3] == 1, 0.1 * first[t], 0.0)
                f_sum[i, ds(t), :] = total[t]

    def inner(i, _):
        at(i, lambda j, t: f[j, i - 1, ds(t), :], lambda j, t: f[j, i + 1, ds(t), :])
        return 0

    at(0, lambda j, t: jnp.where(even_c, c1[j, ds(t), :], c0[j, ds(t), :]), lambda j, t: f[j, 1, ds(t), :])
    lax.fori_loop(1, ni - 1, inner, 0)
    at(ni - 1, lambda j, t: f[j, ni - 2, ds(t), :], lambda j, t: jnp.where(even_c, c0[j, ds(t), :], c1[j, ds(t), :]))
    if not last:
        write_faces(place, out, s_c0, s_c1, s_k, earlier)


def totals_body(place, g_a, s_a, g_b, s_b, c0_a, c1_a, c0_b, c1_b, ks, out, kl, kh):
    ni, nk = g_a.shape[:2]
    nj = ks.shape[0]
    tiles = nk // TILE
    wide = left((ni, 128))
    row = lax.broadcasted_iota(jnp.int32, (TILE, 128), 0)
    top, bottom = row == 0, row == TILE - 1
    even_c = place[1] == 0
    across = ks[0]
    for j in range(1, nj):
        across = across + ks[j]
    for h, (g, s, c0, c1) in enumerate(((g_a, s_a, c0_a, c1_a), (g_b, s_b, c0_b, c1_b))):
        x = across if h else swap(across)
        kl[h] = jnp.where(wide, jnp.where(place[2] == 1, x, 0.0), swap(s[:, nk - 1, :]))
        kh[h] = jnp.where(wide, swap(s[:, 0, :]), jnp.where(place[2] == 0, x, 0.0))
        ends = []
        for t in range(tiles):
            part = pl.ds(t * TILE, TILE)
            sum0, sum1 = c0[0, part, :], c1[0, part, :]
            for j in range(1, nj):
                sum0, sum1 = sum0 + c0[j, part, :], sum1 + c1[j, part, :]
            ends.append((jnp.where(even_c, sum1, sum0), jnp.where(even_c, sum0, sum1)))
        for i in range(ni):
            low = jnp.broadcast_to(kl[h, pl.ds(i, 1), :], (TILE, 128))
            high = jnp.broadcast_to(kh[h, pl.ds(i, 1), :], (TILE, 128))
            for t in range(tiles):
                part = pl.ds(t * TILE, TILE)
                mid = s[i, part, :]
                below = s[i - 1, part, :] if i else ends[t][0]
                above = s[i + 1, part, :] if i + 1 < ni else ends[t][1]
                if t:
                    before = s[i, pl.ds(t * TILE - 1, TILE), :]
                else:
                    before = jnp.where(top, low, pltpu.roll(mid, 1, 0))
                if t + 1 < tiles:
                    after = s[i, pl.ds(t * TILE + 1, TILE), :]
                else:
                    after = jnp.where(bottom, high, pltpu.roll(mid, TILE - 1, 0))
                around = (mid + mid) + (below + above) + (before + after)
                out[i, pl.ds(h * nk + t * TILE, TILE), :] = g[i, part, :] + 0.1 * around


def prefix_body(g, out):
    n = g.shape[0]
    state = jnp.zeros(g.shape[1:], jnp.float32)
    for d in range(n):
        out[d] = state
        if d + 1 < n:
            state = state + g[d]


GROUP = 2


def finish_body(scale, fa, fb, base, fix_a, fix_b, potential, field, pot, end, sems):
    nj, ni, nk = fa.shape[:3]

    def copies(g):
        part = pl.ds(g * GROUP, GROUP)
        return (
            pltpu.make_async_copy(pot.at[:, part], potential.at[:, part], sems.at[g, 0]),
            pltpu.make_async_copy(end.at[:, part], field.at[:, part], sems.at[g, 1]),
        )

    def at(g, _):
        for n in range(GROUP):
            i = g * GROUP + n
            for t in range(nk // TILE):
                lo, hi = pl.ds(t * TILE, TILE), pl.ds(nk + t * TILE, TILE)
                acc0, acc1 = exchange_halves(base[i, lo, :] + fix_a[i, lo, :], base[i, hi, :] + fix_b[i, lo, :])
                for j in range(nj):
                    v0, v1 = exchange_halves(fa[j, i, lo, :], fb[j, i, lo, :])
                    end[j, i, lo, :] = v0
                    end[j, i, hi, :] = v1
                    acc0, acc1 = acc0 + v0, acc1 + v1
                    pot[j, i, lo, :] = acc0 * scale
                    pot[j, i, hi, :] = acc1 * scale
        for copy in copies(g):
            copy.start()
        return 0

    def finished(g, _):
        for copy in copies(g):
            copy.wait()
        return 0

    lax.fori_loop(0, ni // GROUP, at, 0)
    lax.fori_loop(0, ni // GROUP, finished, 0)


def pairs(size, start):
    out = []
    for i in range(start, size - 1, 2):
        out += [(i, i + 1), (i + 1, i)]
    return out


KINDS = (("r1", "c1", "c0", "r0"), ("k", "r1", "c1", "c0", "r0"))
LAST = (("r1", "c1", "c0", "r0"), ("c1", "c0", "k", "r1", "r0"))


def kinds(step, h):
    return (LAST if step == STEPS - 1 else KINDS)[h]


def exchange(faces, step, h):
    r0, r1, c0, c1, k = faces
    rows, cols, slabs = lax.axis_size("rows"), lax.axis_size("cols"), lax.axis_size("slabs")
    sends = {
        "k": (k, "slabs", pairs(slabs, 0)),
        "c0": (c0, "cols", pairs(cols, 0)),
        "c1": (c1, "cols", pairs(cols, 1)),
        "r0": (r0, "rows", pairs(rows, 0)),
        "r1": (r1, "rows", pairs(rows, 1)),
    }
    got = {}
    for kind in kinds(step, h):
        got[kind] = lax.ppermute(*sends[kind])
    return [got[kind] for kind in ("r0", "r1", "c0", "c1")], got.get("k")


def on_device(field_values, crowding):
    nj, ni, nk, nl = field_values.shape
    half = (nj, ni, nk // 2, nl)
    faces = [(ni, nk // 2, nl)] * 2 + [(nj, nk // 2, nl)] * 2 + [(nj, ni, nl)]
    row = lax.axis_index("rows")
    place = jnp.stack([row % 2, lax.axis_index("cols") % 2, lax.axis_index("slabs"), row == 0])
    place = place.astype(jnp.int32)
    sent = pl.pallas_call(
        pack_faces,
        out_shape=[jax.ShapeDtypeStruct(shape, jnp.float32) for shape in faces[:4] * 2 + faces[4:]],
        in_specs=[SMEM, pl.BlockSpec(memory_space=pltpu.MemorySpace.HBM)],
        scratch_shapes=[pltpu.VMEM((ni, nk, nl), jnp.float32)] * 2
        + [pltpu.VMEM((nj, nk, nl), jnp.float32)] * 2
        + [pltpu.VMEM((nj, ni, TILE, nl), jnp.float32)] * 2
        + [pltpu.SemaphoreType.DMA((6,))],
        compiler_params=pltpu.CompilerParams(vmem_limit_bytes=16 * 1024 * 1024),
    )(place, pltpu.with_memory_space_constraint(field_values, pltpu.MemorySpace.HBM))
    sent = [[*sent[:4], None], sent[4:]]
    halos = [None, None]
    for h in range(2):
        halos[h], across = exchange(sent[h], 0, h)
    f = list(call(pack_field, [half, half], (field_values,)))
    c = call(pack_crowding, [half, half], (crowding,))
    scratch = [(nj, ni, nl)] * 2
    sums, fix, other = [None, None], [None, None], None
    rows = lax.axis_size("rows")
    for step in range(STEPS):
        kind = {STEPS - 1: "last", STEPS - 2: "sums"}.get(step, "plain")
        last = kind == "last"
        if last:
            total = call(
                totals_body,
                [(ni, nk, nl)],
                (place, *sums[0], *sums[1], *halos[0][2:], *halos[1][2:], across),
                [(2, ni, nl)] * 2,
                in_specs=[SMEM] + [VMEM] * 9,
            )[0]
            total = total.reshape(rows, ni * nk // rows, nl)
            gathered = lax.all_to_all(total, "rows", 0, 0, tiled=True)
            gathered, place = lax.optimization_barrier((gathered, place))
            before = call(prefix_body, [gathered.shape], (gathered,))[0]
        for h in range(2):
            args = (place, f[h], c[h], *halos[h], across) + ((other,) if h and not last else ())
            plane = (ni, nk // 2, nl)
            outs = [half] + {"last": [plane], "sums": faces + [plane] * 2, "plain": faces}[kind]
            res = call(
                functools.partial(step_body, kind, h),
                outs,
                args,
                scratch,
                in_specs=[SMEM] + [VMEM] * (len(args) - 1),
            )
            f[h] = res[0]
            if last:
                fix[h] = res[1]
            else:
                sums[h] = res[6:]
                other = res[5]
                halos[h], got = exchange(res[1:6], step + 1, h)
        if not last:
            across = got
    before, *f = lax.optimization_barrier((before, *f))
    base = lax.all_to_all(before, "rows", 0, 0, tiled=True).reshape(ni, nk, nl)
    potential, field = pl.pallas_call(
        functools.partial(finish_body, 1.0 / (nj * rows)),
        out_shape=[jax.ShapeDtypeStruct(field_values.shape, jnp.float32)] * 2,
        in_specs=[VMEM] * 5,
        out_specs=[pl.BlockSpec(memory_space=pltpu.MemorySpace.HBM)] * 2,
        scratch_shapes=[pltpu.VMEM(field_values.shape, jnp.float32)] * 2
        + [pltpu.SemaphoreType.DMA((ni // GROUP, 2))],
        compiler_params=pltpu.CompilerParams(vmem_limit_bytes=16 * 1024 * 1024),
    )(*near([f[0], f[1], base, *fix]))
    return potential, field


def solution(mesh):
    spec = P(("trial", "rows"), "cols", "slabs", None)
    return jax.shard_map(on_device, mesh=mesh, in_specs=(spec, spec), out_specs=(spec, spec), check_vma=False)
```

```python
import functools

import jax
import jax.numpy as jnp
from jax import lax
from jax.experimental import pallas as pl
from jax.experimental.pallas import tpu as pltpu
from jax.sharding import PartitionSpec as P


STEPS = 3
HALF = 64
TILE = 8
VMEM = pl.BlockSpec(memory_space=pltpu.MemorySpace.VMEM)
SMEM = pl.BlockSpec(memory_space=pltpu.MemorySpace.SMEM)


def near(args):
    return [pltpu.with_memory_space_constraint(a, pltpu.MemorySpace.VMEM) if a.size > 8 else a for a in args]


def call(body, outs, args, scratch=(), limit=16, **more):
    args = near(args)
    return pl.pallas_call(
        body,
        out_shape=[jax.ShapeDtypeStruct(s, jnp.float32) for s in outs],
        scratch_shapes=[pltpu.VMEM(s, jnp.float32) for s in scratch],
        compiler_params=pltpu.CompilerParams(vmem_limit_bytes=limit * 1024 * 1024),
        **more,
    )(*args)


def left(shape=(TILE, 128)):
    return lax.broadcasted_iota(jnp.int32, shape, len(shape) - 1) < HALF


def swap(v):
    return pltpu.roll(v, HALF, v.ndim - 1)


def exchange_halves(a, b):
    m = left()
    moved = swap(jnp.where(m, b, a))
    return jnp.where(m, a, moved), jnp.where(m, moved, b)


def pack_tiles(ref, j, i, t, nk):
    a = ref[j, i, pl.ds(t * TILE, TILE), :]
    b = ref[j, i, pl.ds(nk // 2 + t * TILE, TILE), :]
    return exchange_halves(a, b)


def edge_rows(place, block, j):
    nk = block.shape[2]
    return jnp.where(place[2] == 0, block[j, :, nk - 1, :], block[j, :, 0, :])


def write_faces(place, out, s_c0, s_c1, s_k, other):
    nj, ni = out.shape[:2]
    wide = left((ni, 128))
    for j in range(nj):
        first, last = out[j, 0], out[j, ni - 1]
        s_c0[j] = jnp.where(place[1] == 0, last, first)
        s_c1[j] = jnp.where(place[1] == 0, first, last)
        rows = edge_rows(place, out, j)
        if other is not None:
            mine = swap(rows)
            rows = jnp.where(place[2] == 0, jnp.where(wide, mine, other[j]), jnp.where(wide, other[j], mine))
        s_k[j] = rows


def pack_faces(place, f, *rest):
    sa, sb, s_k = rest[:4], rest[4:8], rest[8]
    rlo, rhi, clo, chi, klo, khi, sems = rest[9:]
    nj, ni, nk = f.shape[:3]
    copies = [
        pltpu.make_async_copy(part, into, sems.at[n])
        for n, (part, into) in enumerate(
            (
                (f.at[0], rlo),
                (f.at[nj - 1], rhi),
                (f.at[:, 0], clo),
                (f.at[:, ni - 1], chi),
                (f.at[:, :, pl.ds(0, TILE)], klo),
                (f.at[:, :, pl.ds(nk - TILE, TILE)], khi),
            )
        )
    ]
    for copy in copies:
        copy.start()

    def face(n, low, high, even, slot):
        for t in range(nk // 2 // TILE):
            lo, hi = pl.ds(t * TILE, TILE), pl.ds(nk // 2 + t * TILE, TILE)
            first = exchange_halves(low[n, lo, :], low[n, hi, :])
            last = exchange_halves(high[n, lo, :], high[n, hi, :])
            for s, v, w in zip((sa, sb), first, last):
                s[slot][n, lo, :] = jnp.where(even, w, v)
                s[slot + 1][n, lo, :] = jnp.where(even, v, w)

    def along(pair, _):
        for n in range(2):
            face(2 * pair + n, rlo, rhi, place[0] == 0, 0)
        return 0

    copies[0].wait()
    copies[1].wait()
    lax.fori_loop(0, ni // 2, along, 0)
    for copy in copies[2:]:
        copy.wait()
    for j in range(nj):
        face(j, clo, chi, place[1] == 0, 2)
        s_k[j] = jnp.where(place[2] == 0, swap(khi[j, :, TILE - 1, :]), klo[j, :, 0, :])


def pack_field(f, fa, fb):
    nj, ni, nk = f.shape[:3]

    def at(i, _):
        for j in range(nj):
            for t in range(nk // 2 // TILE):
                a, b = pack_tiles(f, j, i, t, nk)
                fa[j, i, pl.ds(t * TILE, TILE), :] = a
                fb[j, i, pl.ds(t * TILE, TILE), :] = b
        return 0

    lax.fori_loop(0, ni, at, 0)


def pack_crowding(c, ca, cb):
    nj, ni, nk = c.shape[:3]

    def at(i, _):
        for j in range(nj):
            for t in range(nk // 2 // TILE):
                a, b = pack_tiles(c, j, i, t, nk)
                ca[j, i, pl.ds(t * TILE, TILE), :] = 0.2 * a
                cb[j, i, pl.ds(t * TILE, TILE), :] = 0.2 * b
        return 0

    lax.fori_loop(0, ni, at, 0)


def step_body(kind, h, place, f, c, r0, r1, c0, c1, ks, *rest):
    rest = list(rest)
    last, with_sums = kind == "last", kind == "sums"
    earlier = rest.pop(0) if h and not last else None
    out = rest.pop(0)
    if last:
        fix = rest.pop(0)
    else:
        s_r0, s_r1, s_c0, s_c1, s_k = rest[:5]
        rest = rest[5:]
        if with_sums:
            g_sum, f_sum = rest[:2]
            rest = rest[2:]
    kl, kh = rest
    nj, ni, nk = f.shape[:3]
    tiles = nk // TILE
    wide = left((ni, 128))
    for j in range(nj):
        x = ks[j] if h else swap(ks[j])
        low_side = jnp.where(place[2] == 1, x, 0.0)
        high_side = jnp.where(place[2] == 0, x, 0.0)
        kl[j] = jnp.where(wide, low_side, swap(f[j, :, nk - 1, :]))
        kh[j] = jnp.where(wide, swap(f[j, :, 0, :]), high_side)
    row = lax.broadcasted_iota(jnp.int32, (TILE, 128), 0)
    top, bottom = row == 0, row == TILE - 1
    even_r, even_c = place[0] == 0, place[1] == 0

    def ds(t):
        return pl.ds(t * TILE, TILE)

    def at(i, below, above):
        down = [jnp.where(even_r, r1[i, ds(t), :], r0[i, ds(t), :]) for t in range(tiles)]
        mid = [f[0, i, ds(t), :] for t in range(tiles)]
        first, grown, total = [None] * tiles, [None] * tiles, [None] * tiles
        if last:
            for t in range(tiles):
                fix[i, ds(t), :] = jnp.where(place[3] == 0, 0.1 * (mid[t] - down[t]), 0.0)
        for j in range(nj):
            if j + 1 < nj:
                up = [f[j + 1, i, ds(t), :] for t in range(tiles)]
            else:
                up = [jnp.where(even_r, r0[i, ds(t), :], r1[i, ds(t), :]) for t in range(tiles)]
            low = jnp.broadcast_to(kl[j, pl.ds(i, 1), :], (TILE, 128))
            high = jnp.broadcast_to(kh[j, pl.ds(i, 1), :], (TILE, 128))
            for t in range(tiles):
                if t:
                    before = f[j, i, pl.ds(t * TILE - 1, TILE), :]
                else:
                    before = jnp.where(top, low, pltpu.roll(mid[t], 1, 0))
                if t + 1 < tiles:
                    after = f[j, i, pl.ds(t * TILE + 1, TILE), :]
                else:
                    after = jnp.where(bottom, high, pltpu.roll(mid[t], TILE - 1, 0))
                around = (down[t] + up[t]) + (below(j, t) + above(j, t)) + (before + after)
                v = mid[t] * (0.6 - c[j, i, ds(t), :] * mid[t]) + 0.1 * around
                out[j, i, ds(t), :] = v
                if j == 0:
                    first[t] = v
                elif j == nj - 1 and not last:
                    s_r0[i, ds(t), :] = jnp.where(even_r, v, first[t])
                    s_r1[i, ds(t), :] = jnp.where(even_r, first[t], v)
                if with_sums:
                    own = v * (0.6 - c[j, i, ds(t), :] * v)
                    grown[t] = own if j == 0 else grown[t] + own
                    total[t] = v if j == 0 else total[t] + v
            down, mid = mid, up
        if with_sums:
            for t in range(tiles):
                g_sum[i, ds(t), :] = grown[t] - jnp.where(place[3] == 1, 0.1 * first[t], 0.0)
                f_sum[i, ds(t), :] = total[t]

    def inner(i, _):
        at(i, lambda j, t: f[j, i - 1, ds(t), :], lambda j, t: f[j, i + 1, ds(t), :])
        return 0

    at(0, lambda j, t: jnp.where(even_c, c1[j, ds(t), :], c0[j, ds(t), :]), lambda j, t: f[j, 1, ds(t), :])
    lax.fori_loop(1, ni - 1, inner, 0)
    at(ni - 1, lambda j, t: f[j, ni - 2, ds(t), :], lambda j, t: jnp.where(even_c, c0[j, ds(t), :], c1[j, ds(t), :]))
    if not last:
        write_faces(place, out, s_c0, s_c1, s_k, earlier)


def pack_both(f, c, fa, fb, ca, cb):
    pack_field(f, fa, fb)
    pack_crowding(c, ca, cb)


def totals_body(place, g_a, s_a, g_b, s_b, c0_a, c1_a, c0_b, c1_b, ks, out, kl, kh):
    ni, nk = g_a.shape[:2]
    nj = ks.shape[0]
    tiles = nk // TILE
    wide = left((ni, 128))
    row = lax.broadcasted_iota(jnp.int32, (TILE, 128), 0)
    top, bottom = row == 0, row == TILE - 1
    even_c = place[1] == 0
    across = ks[0]
    for j in range(1, nj):
        across = across + ks[j]
    for h, (g, s, c0, c1) in enumerate(((g_a, s_a, c0_a, c1_a), (g_b, s_b, c0_b, c1_b))):
        x = across if h else swap(across)
        kl[h] = jnp.where(wide, jnp.where(place[2] == 1, x, 0.0), swap(s[:, nk - 1, :]))
        kh[h] = jnp.where(wide, swap(s[:, 0, :]), jnp.where(place[2] == 0, x, 0.0))
        ends = []
        for t in range(tiles):
            part = pl.ds(t * TILE, TILE)
            sum0, sum1 = c0[0, part, :], c1[0, part, :]
            for j in range(1, nj):
                sum0, sum1 = sum0 + c0[j, part, :], sum1 + c1[j, part, :]
            ends.append((jnp.where(even_c, sum1, sum0), jnp.where(even_c, sum0, sum1)))
        for i in range(ni):
            low = jnp.broadcast_to(kl[h, pl.ds(i, 1), :], (TILE, 128))
            high = jnp.broadcast_to(kh[h, pl.ds(i, 1), :], (TILE, 128))
            for t in range(tiles):
                part = pl.ds(t * TILE, TILE)
                mid = s[i, part, :]
                below = s[i - 1, part, :] if i else ends[t][0]
                above = s[i + 1, part, :] if i + 1 < ni else ends[t][1]
                if t:
                    before = s[i, pl.ds(t * TILE - 1, TILE), :]
                else:
                    before = jnp.where(top, low, pltpu.roll(mid, 1, 0))
                if t + 1 < tiles:
                    after = s[i, pl.ds(t * TILE + 1, TILE), :]
                else:
                    after = jnp.where(bottom, high, pltpu.roll(mid, TILE - 1, 0))
                around = (mid + mid) + (below + above) + (before + after)
                out[i, pl.ds(h * nk + t * TILE, TILE), :] = g[i, part, :] + 0.1 * around


def prefix_body(g, out):
    n = g.shape[0]
    state = jnp.zeros(g.shape[1:], jnp.float32)
    for d in range(n):
        out[d] = state
        if d + 1 < n:
            state = state + g[d]


GROUP = 2


def finish_body(scale, fa, fb, base, fix_a, fix_b, potential, field, pot, end, sems):
    nj, ni, nk = fa.shape[:3]

    def copies(g):
        part = pl.ds(g * GROUP, GROUP)
        return (
            pltpu.make_async_copy(pot.at[:, part], potential.at[:, part], sems.at[g, 0]),
            pltpu.make_async_copy(end.at[:, part], field.at[:, part], sems.at[g, 1]),
        )

    def at(g, _):
        for n in range(GROUP):
            i = g * GROUP + n
            for t in range(nk // TILE):
                lo, hi = pl.ds(t * TILE, TILE), pl.ds(nk + t * TILE, TILE)
                acc0, acc1 = exchange_halves(base[i, lo, :] + fix_a[i, lo, :], base[i, hi, :] + fix_b[i, lo, :])
                for j in range(nj):
                    v0, v1 = exchange_halves(fa[j, i, lo, :], fb[j, i, lo, :])
                    end[j, i, lo, :] = v0
                    end[j, i, hi, :] = v1
                    acc0, acc1 = acc0 + v0, acc1 + v1
                    pot[j, i, lo, :] = acc0 * scale
                    pot[j, i, hi, :] = acc1 * scale
        for copy in copies(g):
            copy.start()
        return 0

    def finished(g, _):
        for copy in copies(g):
            copy.wait()
        return 0

    lax.fori_loop(0, ni // GROUP, at, 0)
    lax.fori_loop(0, ni // GROUP, finished, 0)


def pairs(size, start):
    out = []
    for i in range(start, size - 1, 2):
        out += [(i, i + 1), (i + 1, i)]
    return out


KINDS = (("r1", "c1", "c0", "r0"), ("k", "r1", "c1", "c0", "r0"))
LAST = (("r1", "c1", "c0", "r0"), ("c1", "c0", "k", "r1", "r0"))


def kinds(step, h):
    return (LAST if step == STEPS - 1 else KINDS)[h]


def exchange(faces, step, h):
    r0, r1, c0, c1, k = faces
    rows, cols, slabs = lax.axis_size("rows"), lax.axis_size("cols"), lax.axis_size("slabs")
    sends = {
        "k": (k, "slabs", pairs(slabs, 0)),
        "c0": (c0, "cols", pairs(cols, 0)),
        "c1": (c1, "cols", pairs(cols, 1)),
        "r0": (r0, "rows", pairs(rows, 0)),
        "r1": (r1, "rows", pairs(rows, 1)),
    }
    got = {}
    for kind in kinds(step, h):
        got[kind] = lax.ppermute(*sends[kind])
    return [got[kind] for kind in ("r0", "r1", "c0", "c1")], got.get("k")


def on_device(field_values, crowding):
    nj, ni, nk, nl = field_values.shape
    half = (nj, ni, nk // 2, nl)
    faces = [(ni, nk // 2, nl)] * 2 + [(nj, nk // 2, nl)] * 2 + [(nj, ni, nl)]
    row = lax.axis_index("rows")
    place = jnp.stack([row % 2, lax.axis_index("cols") % 2, lax.axis_index("slabs"), row == 0])
    place = place.astype(jnp.int32)
    sent = pl.pallas_call(
        pack_faces,
        out_shape=[jax.ShapeDtypeStruct(shape, jnp.float32) for shape in faces[:4] * 2 + faces[4:]],
        in_specs=[SMEM, pl.BlockSpec(memory_space=pltpu.MemorySpace.HBM)],
        scratch_shapes=[pltpu.VMEM((ni, nk, nl), jnp.float32)] * 2
        + [pltpu.VMEM((nj, nk, nl), jnp.float32)] * 2
        + [pltpu.VMEM((nj, ni, TILE, nl), jnp.float32)] * 2
        + [pltpu.SemaphoreType.DMA((6,))],
        compiler_params=pltpu.CompilerParams(vmem_limit_bytes=16 * 1024 * 1024),
    )(place, pltpu.with_memory_space_constraint(field_values, pltpu.MemorySpace.HBM))
    sent = [[*sent[:4], None], sent[4:]]
    halos = [None, None]
    for h in range(2):
        halos[h], across = exchange(sent[h], 0, h)
    packed = call(pack_both, [half] * 4, (field_values, crowding))
    f, c = list(packed[:2]), packed[2:]
    scratch = [(nj, ni, nl)] * 2
    sums, fix, other = [None, None], [None, None], None
    rows = lax.axis_size("rows")
    for step in range(STEPS):
        kind = {STEPS - 1: "last", STEPS - 2: "sums"}.get(step, "plain")
        last = kind == "last"
        if last:
            total = call(
                totals_body,
                [(ni, nk, nl)],
                (place, *sums[0], *sums[1], *halos[0][2:], *halos[1][2:], across),
                [(2, ni, nl)] * 2,
                in_specs=[SMEM] + [VMEM] * 9,
            )[0]
            total = total.reshape(rows, ni * nk // rows, nl)
            gathered = lax.all_to_all(total, "rows", 0, 0, tiled=True)
            gathered, place = lax.optimization_barrier((gathered, place))
            before = call(prefix_body, [gathered.shape], (gathered,))[0]
        for h in range(2):
            args = (place, f[h], c[h], *halos[h], across) + ((other,) if h and not last else ())
            plane = (ni, nk // 2, nl)
            outs = [half] + {"last": [plane], "sums": faces + [plane] * 2, "plain": faces}[kind]
            res = call(
                functools.partial(step_body, kind, h),
                outs,
                args,
                scratch,
                in_specs=[SMEM] + [VMEM] * (len(args) - 1),
            )
            f[h] = res[0]
            if last:
                fix[h] = res[1]
            else:
                sums[h] = res[6:]
                other = res[5]
                halos[h], got = exchange(res[1:6], step + 1, h)
        if not last:
            across = got
    before, *f = lax.optimization_barrier((before, *f))
    base = lax.all_to_all(before, "rows", 0, 0, tiled=True).reshape(ni, nk, nl)
    potential, field = pl.pallas_call(
        functools.partial(finish_body, 1.0 / (nj * rows)),
        out_shape=[jax.ShapeDtypeStruct(field_values.shape, jnp.float32)] * 2,
        in_specs=[VMEM] * 5,
        out_specs=[pl.BlockSpec(memory_space=pltpu.MemorySpace.HBM)] * 2,
        scratch_shapes=[pltpu.VMEM(field_values.shape, jnp.float32)] * 2
        + [pltpu.SemaphoreType.DMA((ni // GROUP, 2))],
        compiler_params=pltpu.CompilerParams(vmem_limit_bytes=16 * 1024 * 1024),
    )(*near([f[0], f[1], base, *fix]))
    return potential, field


def solution(mesh):
    spec = P(("trial", "rows"), "cols", "slabs", None)
    return jax.shard_map(on_device, mesh=mesh, in_specs=(spec, spec), out_specs=(spec, spec), check_vma=False)
```
